768 devices in a mesh: rows: 64 (over x, y, core), cols: 12 (over z).
Axes of the slice: x: 4, y: 8, z: 12, core: 2. Of those that a mesh axis runs over, the one named last changes fastest.
Arguments:
- basis: bfloat16 [786432, 512], P(('rows', 'cols')), may hold values from -6 to 6
- blocks: bfloat16 [6144, 8, 128, 128], P(('rows', 'cols')), may hold values from -0.1875 to 0.1875
- neighbours: int32 [6144, 8], P(('rows', 'cols')), may hold values from 0 to 6143, as said below
- counts: int32 [6144], P(('rows', 'cols')), may hold values from 3 to 8
- rotation: bfloat16 [512, 256], replicated, may hold values from -0.25 to 0.25
- ritz_values: float32 [256], replicated, may hold values from -2 to 2
Outputs:
- ritz: bfloat16 [786432, 256], P(('rows', 'cols'))
- ritz_image: bfloat16 [786432, 256], P(('rows', 'cols'))
- gram: float32 [512, 512], P('rows')
- projected: float32 [512, 512], P('rows')
- res_norm: float32 [256], replicated
The draws below stay inside these ranges and needn't reach their ends.
Inputs may be any that keep to these rules, and one draw needn't show every extreme that they name: `neighbours`: every entry of row block b lies among the blocks of b's device and the one block just before and just after them: from 8 * (b // 8) - 1 to 8 * (b // 8) + 8; slot 0 is b itself; entries may repeat; entries at slots from counts[b] on are padding. `counts`: at least three slots are live.
All inputs are finite; a program needn't handle non-finite values.
Results may differ from the reference program's by a relative error of at most 0.015.
Values may be sent and summed in bfloat16 or wider, within the bound.
No kernel may reach another device: no remote copies, remote signals or barrier semaphores. Data moves between devices by JAX's collectives and lax.ppermute only.
A program may use at most 64 MiB of HBM per device.

```python
import jax
import jax.numpy as jnp
from jax import lax

BS = 128
NB = 8
NNB = 8
K = 512
M = 256
NBLK = 6144
ROWS = 786432


def draw_neighbours(key, part):
    blk = jnp.arange(NBLK, dtype=jnp.int32)
    owner = blk // NB
    local = blk % NB
    lower = owner * NB - 1
    offsets = jax.random.randint(jax.random.fold_in(key, 7), (NBLK, NNB), 0, NB + 2).astype(jnp.int32)
    entry = lower[:, None] + offsets
    entry = entry.at[:, 0].set(blk)
    entry = entry.at[:, 1].set(jnp.where(local == 0, lower, entry[:, 1]))
    entry = entry.at[:, 2].set(jnp.where(local == NB - 1, lower + NB + 1, entry[:, 2]))
    return jnp.clip(entry, 0, NBLK - 1).astype(jnp.int32)


def set_ends(array, key, smallest, top_value):
    spot = [jax.random.randint(jax.random.fold_in(key, axis), (), 0, length) for axis, length in enumerate(array.shape)]
    longest = array.shape.index(max(array.shape))
    beside = spot[:longest] + [(spot[longest] + 1) % array.shape[longest]] + spot[longest + 1:]
    return array.at[tuple(spot)].set(smallest).at[tuple(beside)].set(top_value)


def block_scale(rng, shape, pieces, least, top_value):
    gain = 1.0
    for position, blocks in pieces:
        steps = jax.random.uniform(jax.random.fold_in(jax.random.fold_in(rng, 6), position), (blocks,), jnp.float32, least / len(pieces), top_value / len(pieces))
        gain = gain * jnp.repeat(jnp.exp(steps), shape[position] // blocks).reshape((-1,) + (1,) * (len(shape) - 1 - position))
    return gain


def centred(rng, extent, width, reach, split=(), held_as=jnp.bfloat16):
    level = block_scale(rng, extent, split, -0.22, 0.18) if split else 1.0
    result = jax.random.normal(rng, extent, jnp.float32) * width * level
    return jnp.minimum(jnp.maximum(result, -reach), reach).astype(held_as)


def setup_inputs(seed: int = 0) -> dict:
    key_of = jax.random.split(jax.random.key(seed), 7)
    return {
        "basis": centred(key_of[0], (ROWS, K), 1.0, 6.0, ((0, 768),)),
        "blocks": centred(key_of[1], (NBLK, NNB, BS, BS), (BS * NNB) ** -0.5, 0.1875, ((0, 768),)),
        "neighbours": draw_neighbours(jax.random.fold_in(key_of[6], 71), 0),
        "counts": set_ends(jax.random.randint(key_of[3], (NBLK,), 3, NNB + 1), jax.random.fold_in(key_of[3], 1), 3, NNB).astype(jnp.int32),
        "rotation": centred(key_of[4], (K, M), K ** -0.5, 0.25),
        "ritz_values": jnp.clip(jax.random.uniform(key_of[5], (M,), jnp.float32, -2.0, 2.0), -2.0, 2.0),
    }


def block_rows(args):
    held, index, vb = (args[0], args[1], args[2])
    total = jnp.zeros((held.shape[0], BS, K), jnp.float32)
    for slot in range(NNB):
        picked = vb[index[:, slot]].astype(jnp.float32)
        total = total + jnp.einsum('brs,bsk->brk', held[:, slot].astype(jnp.float32), picked)
    return total.astype(jnp.bfloat16)

def reference(basis, blocks, neighbours, counts, rotation, ritz_values):
    vb = basis.reshape(NBLK, BS, K)
    live = jnp.arange(NNB, dtype=jnp.int32)[None, :] < counts[:, None]
    masked = jnp.where(live[:, :, None, None], blocks, jnp.zeros_like(blocks))
    groups = NBLK // NB
    image = lax.map(lambda pair: block_rows((pair[0], pair[1], vb)), (masked.reshape(groups, NB, NNB, BS, BS), neighbours.reshape(groups, NB, NNB)))
    image = image.reshape(ROWS, K)
    gram = jnp.dot(basis.T, basis, preferred_element_type=jnp.float32) / ROWS
    projected = jnp.dot(basis.T, image, preferred_element_type=jnp.float32) / ROWS
    ritz_full = jnp.dot(basis, rotation, preferred_element_type=jnp.float32)
    image_full = jnp.dot(image, rotation, preferred_element_type=jnp.float32)
    resid = image_full - ritz_values[None, :] * ritz_full
    res_norm = jnp.sqrt(lax.optimization_barrier(jnp.sum(resid * resid, axis=0)) / ROWS)
    return (ritz_full.astype(jnp.bfloat16), image_full.astype(jnp.bfloat16), gram, projected, res_norm)
```

```python
import jax
import jax.numpy as jnp
from jax import lax
from jax.experimental import pallas as pl
from jax.experimental.pallas import tpu as pltpu
from jax.sharding import Mesh
from jax.sharding import PartitionSpec as P

ROWS = ("rows_0", "rows_1", "rows_2")
ROWS_COLS = ("rows_0", "rows_1", "rows_2", "cols")
LANES = 128
F32 = jnp.float32
BF16 = jnp.bfloat16


def dot(a, b):
    return jnp.dot(a, b, preferred_element_type=F32)


def store_tiles(out_ref, acc_ref, nx, ny, nc, first, per_group):
    tiles = acc_ref.shape[1] // LANES
    for x in range(nx):
        for y in range(ny):
            for c in range(nc):
                row = ((x * ny + y) * nc + c) * 8
                for j in range(0, tiles, 2):
                    pair = jnp.concatenate(
                        [
                            acc_ref[row : row + 8, j * LANES : (j + 1) * LANES],
                            acc_ref[row : row + 8, (j + 1) * LANES : (j + 2) * LANES],
                        ],
                        axis=0,
                    )
                    at = (y * per_group + first + j) * 8
                    out_ref[x * nc + c, at : at + 16, :] = pair.astype(BF16)


def early_kernel(nx, ny, nc, basis_ref, rot_ref, basis_t_ref, gram_ref, ritz_ref, acc_ref):
    basis_t_ref[...] = basis_ref[...].T
    acc_ref[...] = dot(basis_t_ref[...], basis_ref[...])
    store_tiles(gram_ref, acc_ref, nx, ny, nc, 0, acc_ref.shape[1] // LANES)
    ritz_ref[...] = dot(basis_ref[...], rot_ref[...]).astype(BF16)


def late_kernel(
    nx, ny, nc,
    neighbours_ref, counts_ref, blocks_ref, basis_ref, low_ref, high_ref, basis_t_ref, gram_ref,
    rot_ref, values_ref, out_ref, ritz_image_ref, padded_ref, image_ref, acc_ref,
):
    nb, slots, size, _ = blocks_ref.shape
    rows, width = basis_ref.shape
    padded_ref[0:size, :] = low_ref[...]
    padded_ref[size : size + rows, :] = basis_ref[...]
    padded_ref[size + rows :, :] = high_ref[...]
    first = neighbours_ref[0, 0] - 1
    for b in range(nb):
        total = None
        for j in range(0, slots, 2):
            held = []
            picked = []
            for s in (j, j + 1):
                block = blocks_ref[b, s]
                held.append(jnp.where(s < counts_ref[b], block, jnp.zeros_like(block)))
                index = jnp.clip(neighbours_ref[b, s] - first, 0, nb + 1)
                picked.append(padded_ref[pl.ds(pl.multiple_of(index * size, size), size), :])
            part = dot(jnp.concatenate(held, axis=1), jnp.concatenate(picked, axis=0))
            total = part if total is None else total + part
        image_ref[b * size : (b + 1) * size, :] = total.astype(BF16)
    acc_ref[...] = dot(basis_t_ref[...], image_ref[...])
    tiles = width // LANES
    for g in range(nx * nc):
        for y in range(ny):
            at = y * 2 * tiles * 8
            out_ref[g, at : at + tiles * 8, :] = gram_ref[g, y * tiles * 8 : (y + 1) * tiles * 8, :]
    store_tiles(out_ref, acc_ref, nx, ny, nc, tiles, 2 * tiles)
    image_full = dot(image_ref[...], rot_ref[...])
    ritz_image_ref[...] = image_full.astype(BF16)
    resid = image_full - values_ref[...] * dot(basis_ref[...], rot_ref[...])
    squares = jnp.sum(resid * resid, axis=0, keepdims=True)
    parts = squares.shape[1] // LANES
    line = lax.broadcasted_iota(jnp.int32, (16, LANES), 0)
    spread = jnp.zeros((16, LANES), F32)
    for p in range(parts):
        spread = jnp.where(line == p, squares[:, p * LANES : (p + 1) * LANES], spread)
    end = 2 * tiles * 8 * ny
    for g in range(nx * nc):
        out_ref[g, end : end + 16, :] = spread.astype(BF16)


def sum_groups(in_ref):
    total = in_ref[0].astype(F32)
    for i in range(1, in_ref.shape[0]):
        total = total + in_ref[i].astype(F32)
    return total


def split_kernel(in_ref, out_ref):
    total = sum_groups(in_ref).astype(BF16)
    ny = out_ref.shape[0]
    each = out_ref.shape[1] - 16
    for y in range(ny):
        out_ref[y, 0:each, :] = total[y * each : (y + 1) * each]
        out_ref[y, each : each + 16, :] = total[ny * each :]


def repeat_kernel(in_ref, out_ref):
    total = sum_groups(in_ref).astype(BF16)
    for i in range(out_ref.shape[0]):
        out_ref[i] = total


def final_kernel(rows_total, in_ref, gram_ref, projected_ref, res_ref):
    total = sum_groups(in_ref) / rows_total
    tiles = gram_ref.shape[1] // LANES
    for j in range(tiles):
        gram_ref[:, j * LANES : (j + 1) * LANES] = total[j * 8 : (j + 1) * 8]
        projected_ref[:, j * LANES : (j + 1) * LANES] = total[(tiles + j) * 8 : (tiles + j + 1) * 8]
    res_ref[...] = jnp.sqrt(total[2 * tiles * 8 : 2 * tiles * 8 + res_ref.shape[0]])


def halos(basis, width):
    count = lax.axis_size(ROWS_COLS)
    forward = [(i, i + 1) for i in range(count - 1)]
    backward = [(target, source) for source, target in forward]
    low = lax.ppermute(basis[basis.shape[0] - width :], ROWS_COLS, forward)
    high = lax.ppermute(basis[:width], ROWS_COLS, backward)
    return low, high


def exchanged(x, axes):
    return lax.all_to_all(x, axes, split_axis=0, concat_axis=0, tiled=True)


def shape(dims, dtype):
    return jax.ShapeDtypeStruct(dims, dtype)


def body(basis, blocks, neighbours, counts, rotation, ritz_values):
    rows, width = basis.shape
    size = blocks.shape[2]
    kept = rotation.shape[1]
    nx, ny, nc = (lax.axis_size(axis) for axis in ROWS)
    nz = lax.axis_size("cols")
    rows_total = rows * nx * ny * nc * nz
    tiles = width // LANES
    groups = nx * nc
    vmem = pl.BlockSpec(memory_space=pltpu.VMEM)
    smem = pl.BlockSpec(memory_space=pltpu.SMEM)
    low, high = halos(basis, size)
    basis_t, gram_part, ritz = pl.pallas_call(
        lambda *refs: early_kernel(nx, ny, nc, *refs),
        out_shape=(
            shape((width, rows), BF16),
            shape((groups, ny * tiles * 8, LANES), BF16),
            shape((rows, kept), BF16),
        ),
        in_specs=[vmem] * 2,
        out_specs=(vmem,) * 3,
        scratch_shapes=[pltpu.VMEM((width, width), F32)],
        cost_estimate=pl.CostEstimate(
            flops=2 * rows * width * (width + kept), bytes_accessed=4 * rows * width * 2, transcendentals=0
        ),
        name="early",
    )(basis, rotation)
    payload, ritz_image = pl.pallas_call(
        lambda *refs: late_kernel(nx, ny, nc, *refs),
        out_shape=(
            shape((groups, ny * 2 * tiles * 8 + 16, LANES), BF16),
            shape((rows, kept), BF16),
        ),
        in_specs=[smem, smem] + [vmem] * 8,
        out_specs=(vmem,) * 2,
        scratch_shapes=[
            pltpu.VMEM((rows + 2 * size, width), BF16),
            pltpu.VMEM((rows, width), BF16),
            pltpu.VMEM((width, width), F32),
        ],
        cost_estimate=pl.CostEstimate(
            flops=4 * rows * width * 1024, bytes_accessed=8 * rows * width * 2, transcendentals=0
        ),
        name="late",
    )(
        neighbours, counts, blocks, basis, low, high, basis_t, gram_part, rotation,
        ritz_values.reshape(1, kept),
    )
    arrived = exchanged(payload, ("rows_0", "rows_2"))
    each = 2 * tiles * 8 + 16
    split = pl.pallas_call(
        split_kernel,
        out_shape=shape((ny, each, LANES), BF16),
        in_specs=[vmem],
        out_specs=vmem,
        name="split",
    )(arrived)
    repeated = pl.pallas_call(
        repeat_kernel,
        out_shape=shape((nz, each, LANES), BF16),
        in_specs=[vmem],
        out_specs=vmem,
        name="repeated",
    )(exchanged(split, "rows_1"))
    gram, projected, res = pl.pallas_call(
        lambda *refs: final_kernel(rows_total, *refs),
        out_shape=(
            shape((8, width), F32),
            shape((8, width), F32),
            shape((kept // LANES, LANES), F32),
        ),
        in_specs=[vmem],
        out_specs=(vmem,) * 3,
        name="final",
    )(exchanged(repeated, "cols"))
    return ritz, ritz_image, gram, projected, res.reshape(kept)


def solution(mesh):
    finer = Mesh(
        mesh.devices.reshape(4, 8, 2, mesh.shape["cols"]), ("rows_0", "rows_1", "rows_2", "cols")
    )
    return jax.shard_map(
        body,
        mesh=finer,
        in_specs=(
            P(ROWS_COLS, None),
            P(ROWS_COLS, None, None, None),
            P(ROWS_COLS, None),
            P(ROWS_COLS),
            P(),
            P(),
        ),
        out_specs=(P(ROWS_COLS, None), P(ROWS_COLS, None), P(ROWS, None), P(ROWS, None), P()),
        check_vma=False,
    )
```

```python
import jax
import jax.numpy as jnp
from jax import lax
from jax.experimental import pallas as pl
from jax.experimental.pallas import tpu as pltpu
from jax.sharding import Mesh
from jax.sharding import PartitionSpec as P

ROWS = ("rows_0", "rows_1", "rows_2")
ROWS_COLS = ("rows_0", "rows_1", "rows_2", "cols")
LANES = 128
F32 = jnp.float32
BF16 = jnp.bfloat16


def dot(a, b):
    return jnp.dot(a, b, preferred_element_type=F32)


def store_tiles(out_ref, acc_ref, nx, ny, nc, core, first):
    tiles = acc_ref.shape[1] // LANES
    for x in range(nx):
        for y in range(ny):
            row = pl.multiple_of(((x * ny + y) * nc + core) * 8, 8)
            for j in range(0, tiles, 2):
                pair = jnp.concatenate(
                    [
                        acc_ref[pl.ds(row, 8), j * LANES : (j + 1) * LANES],
                        acc_ref[pl.ds(row, 8), (j + 1) * LANES : (j + 2) * LANES],
                    ],
                    axis=0,
                )
                at = (first + j) * 8
                out_ref[x, y, at : at + 16, :] = pair.astype(BF16)


def edges_kernel(basis_ref, held_ref, bottom_ref, top_ref):
    size = bottom_ref.shape[0]
    rows = basis_ref.shape[0]
    held_ref[...] = basis_ref[...]
    bottom_ref[...] = basis_ref[rows - size :, :]
    top_ref[...] = basis_ref[0:size, :]


def early_kernel(nx, ny, nc, basis_ref, basis_t_ref, own_ref, other_ref, acc_ref):
    basis_t_ref[...] = basis_ref[...].T
    acc_ref[...] = dot(basis_t_ref[...], basis_ref[...])
    core = lax.axis_index("rows_2")
    store_tiles(own_ref, acc_ref, nx, ny, nc, core, 0)
    store_tiles(other_ref, acc_ref, nx, ny, nc, nc - 1 - core, 0)


def late_kernel(
    nx, ny, nc,
    neighbours_ref, counts_ref, blocks_ref, basis_ref, low_ref, high_ref, basis_t_ref,
    own_gram_ref, other_gram_ref, rot_ref, values_ref, own_ref, other_ref, image_ref, padded_ref,
    acc_ref,
):
    nb, slots, size, _ = blocks_ref.shape
    rows, width = basis_ref.shape
    padded_ref[0:size, :] = low_ref[...]
    padded_ref[size : size + rows, :] = basis_ref[...]
    padded_ref[size + rows :, :] = high_ref[...]
    first = neighbours_ref[0, 0] - 1
    for b in range(nb):
        total = None
        for j in range(0, slots, 2):
            held = []
            picked = []
            for s in (j, j + 1):
                block = blocks_ref[b, s]
                held.append(jnp.where(s < counts_ref[b], block, jnp.zeros_like(block)))
                index = jnp.clip(neighbours_ref[b, s] - first, 0, nb + 1)
                picked.append(padded_ref[pl.ds(pl.multiple_of(index * size, size), size), :])
            part = dot(jnp.concatenate(held, axis=1), jnp.concatenate(picked, axis=0))
            total = part if total is None else total + part
        image_ref[b * size : (b + 1) * size, :] = total.astype(BF16)
    acc_ref[...] = dot(basis_t_ref[...], image_ref[...])
    tiles = width // LANES
    core = lax.axis_index("rows_2")
    own_ref[:, :, 0 : tiles * 8, :] = own_gram_ref[...]
    other_ref[:, :, 0 : tiles * 8, :] = other_gram_ref[...]
    store_tiles(own_ref, acc_ref, nx, ny, nc, core, tiles)
    store_tiles(other_ref, acc_ref, nx, ny, nc, nc - 1 - core, tiles)
    image_full = dot(image_ref[...], rot_ref[...])
    resid = image_full - values_ref[...] * dot(basis_ref[...], rot_ref[...])
    squares = jnp.sum(resid * resid, axis=0, keepdims=True)
    line = lax.broadcasted_iota(jnp.int32, (8, LANES), 0)
    spread = jnp.zeros((8, LANES), F32)
    for p in range(squares.shape[1] // LANES):
        spread = jnp.where(line == p, squares[:, p * LANES : (p + 1) * LANES], spread)
    lines = jnp.broadcast_to(spread.astype(BF16), (nx, ny, 8, LANES))
    own_ref[:, :, 2 * tiles * 8 :, :] = lines
    other_ref[:, :, 2 * tiles * 8 :, :] = lines


def final_kernel(rows_total, in_ref, gram_ref, projected_ref, res_ref):
    total = in_ref[0].astype(F32)
    for i in range(1, in_ref.shape[0]):
        total = total + in_ref[i].astype(F32)
    total = total / rows_total
    tiles = gram_ref.shape[1] // LANES
    for j in range(tiles):
        gram_ref[:, j * LANES : (j + 1) * LANES] = total[j * 8 : (j + 1) * 8]
        projected_ref[:, j * LANES : (j + 1) * LANES] = total[(tiles + j) * 8 : (tiles + j + 1) * 8]
    res_ref[...] = jnp.sqrt(total[2 * tiles * 8 : 2 * tiles * 8 + res_ref.shape[0]])


def halos(bottom, top):
    count = lax.axis_size(ROWS_COLS)
    forward = [(i, i + 1) for i in range(count - 1)]
    backward = [(target, source) for source, target in forward]
    low = lax.ppermute(bottom, ROWS_COLS, forward)
    high = lax.ppermute(top, ROWS_COLS, backward)
    return low, high


def room(mib):
    return pltpu.CompilerParams(vmem_limit_bytes=mib * 2**20)


def exchanged(x, axes):
    return lax.all_to_all(x, axes, split_axis=0, concat_axis=0, tiled=True)


def summed(x, axes):
    arrived = exchanged(x, axes)
    total = arrived[0].astype(F32)
    for i in range(1, arrived.shape[0]):
        total = total + arrived[i].astype(F32)
    return total


def shape(dims, dtype):
    return jax.ShapeDtypeStruct(dims, dtype)


def body(basis, blocks, neighbours, counts, rotation, ritz_values):
    rows, width = basis.shape
    size = blocks.shape[2]
    kept = rotation.shape[1]
    nx, ny, nc = (lax.axis_size(axis) for axis in ROWS)
    nz = lax.axis_size("cols")
    rows_total = rows * nx * ny * nc * nz
    tiles = width // LANES
    vmem = pl.BlockSpec(memory_space=pltpu.VMEM)
    smem = pl.BlockSpec(memory_space=pltpu.SMEM)
    held, bottom, top = pl.pallas_call(
        edges_kernel,
        out_shape=(shape(basis.shape, BF16), shape((size, width), BF16), shape((size, width), BF16)),
        in_specs=[vmem],
        out_specs=(vmem,) * 3,
        compiler_params=room(8),
        name="edges",
    )(basis)
    low, high = halos(bottom, top)
    basis_t, own_gram, other_gram = pl.pallas_call(
        lambda *refs: early_kernel(nx, ny, nc, *refs),
        out_shape=(
            shape((width, rows), BF16),
            shape((nx, ny, tiles * 8, LANES), BF16),
            shape((nx, ny, tiles * 8, LANES), BF16),
        ),
        in_specs=[vmem],
        out_specs=(vmem,) * 3,
        scratch_shapes=[pltpu.VMEM((width, width), F32)],
        cost_estimate=pl.CostEstimate(
            flops=2 * rows * width * width, bytes_accessed=4 * rows * width * 2, transcendentals=0
        ),
        name="early",
        compiler_params=room(16),
    )(held)
    each = 2 * tiles * 8 + 8
    own, other, image = pl.pallas_call(
        lambda *refs: late_kernel(nx, ny, nc, *refs),
        out_shape=(
            shape((nx, ny, each, LANES), BF16),
            shape((nx, ny, each, LANES), BF16),
            shape((rows, width), BF16),
        ),
        in_specs=[smem, smem] + [vmem] * 9,
        out_specs=(vmem,) * 3,
        scratch_shapes=[
            pltpu.VMEM((rows + 2 * size, width), BF16),
            pltpu.VMEM((width, width), F32),
        ],
        cost_estimate=pl.CostEstimate(
            flops=4 * rows * width * 1024, bytes_accessed=8 * rows * width * 2, transcendentals=0
        ),
        name="late",
        compiler_params=room(20),
    )(
        neighbours, counts, blocks, held, low, high, basis_t, own_gram, other_gram, rotation,
        ritz_values.reshape(1, kept),
    )
    ritz = dot(held, rotation).astype(BF16)
    ritz_image = dot(image, rotation).astype(BF16)
    partner = lax.ppermute(other, "rows_2", [(i, nc - 1 - i) for i in range(nc)])
    part = (own.astype(F32) + partner.astype(F32)).astype(BF16)
    part = summed(part, "rows_0").astype(BF16)
    part = summed(part, "rows_1").astype(BF16)
    every = exchanged(jnp.broadcast_to(part[None], (nz, each, LANES)), "cols")
    gram, projected, res = pl.pallas_call(
        lambda *refs: final_kernel(rows_total, *refs),
        out_shape=(
            shape((8, width), F32),
            shape((8, width), F32),
            shape((kept // LANES, LANES), F32),
        ),
        in_specs=[vmem],
        out_specs=(vmem,) * 3,
        compiler_params=room(8),
        name="final",
    )(every)
    return ritz, ritz_image, gram, projected, res.reshape(kept)


def solution(mesh):
    finer = Mesh(
        mesh.devices.reshape(4, 8, 2, mesh.shape["cols"]), ("rows_0", "rows_1", "rows_2", "cols")
    )
    return jax.shard_map(
        body,
        mesh=finer,
        in_specs=(
            P(ROWS_COLS, None),
            P(ROWS_COLS, None, None, None),
            P(ROWS_COLS, None),
            P(ROWS_COLS),
            P(),
            P(),
        ),
        out_specs=(P(ROWS_COLS, None), P(ROWS_COLS, None), P(ROWS, None), P(ROWS, None), P()),
        check_vma=False,
    )
```

```python
import jax
import jax.numpy as jnp
from jax import lax
from jax.experimental import pallas as pl
from jax.experimental.pallas import tpu as pltpu
from jax.sharding import Mesh
from jax.sharding import PartitionSpec as P

ROWS = ("rows_0", "rows_1", "rows_2")
ROWS_COLS = ("rows_0", "rows_1", "rows_2", "cols")
LANES = 128
F32 = jnp.float32
BF16 = jnp.bfloat16


def dot(a, b):
    return jnp.dot(a, b, preferred_element_type=F32)


def store_tiles(out_ref, acc_ref, nx, ny, nc, core, first):
    tiles = acc_ref.shape[1] // LANES
    for x in range(nx):
        for y in range(ny):
            row = pl.multiple_of(((x * ny + y) * nc + core) * 8, 8)
            for j in range(0, tiles, 2):
                pair = jnp.concatenate(
                    [
                        acc_ref[pl.ds(row, 8), j * LANES : (j + 1) * LANES],
                        acc_ref[pl.ds(row, 8), (j + 1) * LANES : (j + 2) * LANES],
                    ],
                    axis=0,
                )
                at = (first + j) * 8
                out_ref[x, y, at : at + 16, :] = pair.astype(BF16)


def edges_kernel(basis_ref, held_ref, bottom_ref, top_ref):
    size = bottom_ref.shape[0]
    rows = basis_ref.shape[0]
    held_ref[...] = basis_ref[...]
    bottom_ref[...] = basis_ref[rows - size :, :]
    top_ref[...] = basis_ref[0:size, :]


def early_kernel(
    nx, ny, nc, basis_ref, basis_t_ref, own_ref, other_ref, acc_ref
):
    basis_t_ref[...] = basis_ref[...].T
    acc_ref[...] = dot(basis_t_ref[...], basis_ref[...])
    core = lax.axis_index("rows_2")
    store_tiles(own_ref, acc_ref, nx, ny, nc, core, 0)
    store_tiles(other_ref, acc_ref, nx, ny, nc, nc - 1 - core, 0)


def local_kernel(
    neighbours_ref, counts_ref, blocks_ref, basis_ref, rot_ref, local_ref, sums_ref, ritz_ref
):
    ritz_ref[...] = dot(basis_ref[...], rot_ref[...])
    nb, slots, size, _ = blocks_ref.shape
    before = neighbours_ref[0, 0] - 1
    for b in range(nb):
        rows = slice(b * size, (b + 1) * size)
        total = None
        low = jnp.zeros((size, size), F32)
        high = jnp.zeros((size, size), F32)
        for j in range(0, slots, 2):
            held = []
            picked = []
            for s in (j, j + 1):
                index = neighbours_ref[b, s] - before
                live = s < counts_ref[b]
                inside = jnp.logical_and(live, jnp.logical_and(index >= 1, index <= nb))
                block = blocks_ref[b, s]
                held.append(jnp.where(inside, block, jnp.zeros_like(block)))
                at = jnp.clip(index - 1, 0, nb - 1) * size
                picked.append(basis_ref[pl.ds(pl.multiple_of(at, size), size), :])
                wide = block.astype(F32)
                is_low = jnp.logical_and(live, index == 0)
                is_high = jnp.logical_and(live, index == nb + 1)
                low = low + jnp.where(is_low, 1.0, 0.0) * wide
                high = high + jnp.where(is_high, 1.0, 0.0) * wide
            part = dot(jnp.concatenate(held, axis=1), jnp.concatenate(picked, axis=0))
            total = part if total is None else total + part
        local_ref[rows, :] = total
        for side, matrix in enumerate((low, high)):
            first = matrix.astype(BF16)
            rest = (matrix - first.astype(F32)).astype(BF16)
            sums_ref[rows, 2 * side * size : (2 * side + 1) * size] = first
            sums_ref[rows, (2 * side + 1) * size : (2 * side + 2) * size] = rest


def late_kernel(
    nx, ny, nc,
    local_ref, sums_ref, low_ref, high_ref, basis_t_ref, own_gram_ref, other_gram_ref, rot_ref,
    values_ref, ritz_ref, own_ref, other_ref, image_ref, acc_ref,
):
    width = local_ref.shape[1]
    sides = jnp.concatenate([low_ref[...], low_ref[...], high_ref[...], high_ref[...]], axis=0)
    image_ref[...] = (local_ref[...] + dot(sums_ref[...], sides)).astype(BF16)
    acc_ref[...] = dot(basis_t_ref[...], image_ref[...])
    tiles = width // LANES
    core = lax.axis_index("rows_2")
    own_ref[:, :, 0 : tiles * 8, :] = own_gram_ref[...]
    other_ref[:, :, 0 : tiles * 8, :] = other_gram_ref[...]
    store_tiles(own_ref, acc_ref, nx, ny, nc, core, tiles)
    store_tiles(other_ref, acc_ref, nx, ny, nc, nc - 1 - core, tiles)
    image_full = dot(image_ref[...], rot_ref[...])
    resid = image_full - values_ref[...] * ritz_ref[...]
    squares = jnp.sum(resid * resid, axis=0, keepdims=True)
    line = lax.broadcasted_iota(jnp.int32, (8, LANES), 0)
    spread = jnp.zeros((8, LANES), F32)
    for p in range(squares.shape[1] // LANES):
        spread = jnp.where(line == p, squares[:, p * LANES : (p + 1) * LANES], spread)
    lines = jnp.broadcast_to(spread.astype(BF16), (nx, ny, 8, LANES))
    own_ref[:, :, 2 * tiles * 8 :, :] = lines
    other_ref[:, :, 2 * tiles * 8 :, :] = lines


def final_kernel(rows_total, in_ref, gram_ref, projected_ref, res_ref):
    total = in_ref[0].astype(F32)
    for i in range(1, in_ref.shape[0]):
        total = total + in_ref[i].astype(F32)
    total = total / rows_total
    tiles = gram_ref.shape[1] // LANES
    for j in range(tiles):
        gram_ref[:, j * LANES : (j + 1) * LANES] = total[j * 8 : (j + 1) * 8]
        projected_ref[:, j * LANES : (j + 1) * LANES] = total[(tiles + j) * 8 : (tiles + j + 1) * 8]
    res_ref[...] = jnp.sqrt(total[2 * tiles * 8 : 2 * tiles * 8 + res_ref.shape[0]])


def halos(bottom, top):
    count = lax.axis_size(ROWS_COLS)
    forward = [(i, i + 1) for i in range(count - 1)]
    backward = [(target, source) for source, target in forward]
    low = lax.ppermute(bottom, ROWS_COLS, forward)
    high = lax.ppermute(top, ROWS_COLS, backward)
    return low, high


def room(mib):
    return pltpu.CompilerParams(vmem_limit_bytes=mib * 2**20)


def exchanged(x, axes):
    return lax.all_to_all(x, axes, split_axis=0, concat_axis=0, tiled=True)


def summed(x, axes):
    arrived = exchanged(x, axes)
    total = arrived[0].astype(F32)
    for i in range(1, arrived.shape[0]):
        total = total + arrived[i].astype(F32)
    return total


def shape(dims, dtype):
    return jax.ShapeDtypeStruct(dims, dtype)


def body(basis, blocks, neighbours, counts, rotation, ritz_values):
    rows, width = basis.shape
    size = blocks.shape[2]
    kept = rotation.shape[1]
    nx, ny, nc = (lax.axis_size(axis) for axis in ROWS)
    nz = lax.axis_size("cols")
    rows_total = rows * nx * ny * nc * nz
    tiles = width // LANES
    vmem = pl.BlockSpec(memory_space=pltpu.VMEM)
    smem = pl.BlockSpec(memory_space=pltpu.SMEM)
    held, bottom, top = pl.pallas_call(
        edges_kernel,
        out_shape=(shape(basis.shape, BF16), shape((size, width), BF16), shape((size, width), BF16)),
        in_specs=[vmem],
        out_specs=(vmem,) * 3,
        compiler_params=room(8),
        name="edges",
    )(basis)
    low, high = halos(bottom, top)
    basis_t, own_gram, other_gram = pl.pallas_call(
        lambda *refs: early_kernel(nx, ny, nc, *refs),
        out_shape=(
            shape((width, rows), BF16),
            shape((nx, ny, tiles * 8, LANES), BF16),
            shape((nx, ny, tiles * 8, LANES), BF16),
        ),
        in_specs=[vmem],
        out_specs=(vmem,) * 3,
        scratch_shapes=[pltpu.VMEM((width, width), F32)],
        cost_estimate=pl.CostEstimate(
            flops=2 * rows * width * width, bytes_accessed=4 * rows * width * 2, transcendentals=0
        ),
        name="early",
        compiler_params=room(16),
    )(held)
    local, sums, ritz_full = pl.pallas_call(
        local_kernel,
        out_shape=(
            shape((rows, width), F32),
            shape((rows, 4 * size), BF16),
            shape((rows, kept), F32),
        ),
        in_specs=[smem, smem] + [vmem] * 3,
        out_specs=(vmem,) * 3,
        compiler_params=room(16),
        cost_estimate=pl.CostEstimate(
            flops=2 * rows * width * 1024, bytes_accessed=6 * rows * width * 2, transcendentals=0
        ),
        name="local",
    )(neighbours, counts, blocks, held, rotation)
    each = 2 * tiles * 8 + 8
    own, other, image = pl.pallas_call(
        lambda *refs: late_kernel(nx, ny, nc, *refs),
        out_shape=(
            shape((nx, ny, each, LANES), BF16),
            shape((nx, ny, each, LANES), BF16),
            shape((rows, width), BF16),
        ),
        in_specs=[vmem] * 10,
        out_specs=(vmem,) * 3,
        scratch_shapes=[
            pltpu.VMEM((width, width), F32),
        ],
        cost_estimate=pl.CostEstimate(
            flops=4 * rows * width * 1024, bytes_accessed=8 * rows * width * 2, transcendentals=0
        ),
        name="late",
        compiler_params=room(20),
    )(
        local, sums, low, high, basis_t, own_gram, other_gram, rotation,
        ritz_values.reshape(1, kept), ritz_full,
    )
    ritz = dot(held, rotation).astype(BF16)
    ritz_image = dot(image, rotation).astype(BF16)
    partner = lax.ppermute(other, "rows_2", [(i, nc - 1 - i) for i in range(nc)])
    part = (own.astype(F32) + partner.astype(F32)).astype(BF16)
    part = summed(part.reshape(nx * ny, each, LANES), ("rows_0", "rows_1")).astype(BF16)
    every = exchanged(jnp.broadcast_to(part[None], (nz, each, LANES)), "cols")
    gram, projected, res = pl.pallas_call(
        lambda *refs: final_kernel(rows_total, *refs),
        out_shape=(
            shape((8, width), F32),
            shape((8, width), F32),
            shape((kept // LANES, LANES), F32),
        ),
        in_specs=[vmem],
        out_specs=(vmem,) * 3,
        compiler_params=room(8),
        name="final",
    )(every)
    return ritz, ritz_image, gram, projected, res.reshape(kept)


def solution(mesh):
    finer = Mesh(
        mesh.devices.reshape(4, 8, 2, mesh.shape["cols"]), ("rows_0", "rows_1", "rows_2", "cols")
    )
    return jax.shard_map(
        body,
        mesh=finer,
        in_specs=(
            P(ROWS_COLS, None),
            P(ROWS_COLS, None, None, None),
            P(ROWS_COLS, None),
            P(ROWS_COLS),
            P(),
            P(),
        ),
        out_specs=(P(ROWS_COLS, None), P(ROWS_COLS, None), P(ROWS, None), P(ROWS, None), P()),
        check_vma=False,
    )
```
